256 devices in a mesh: task: 32 (over z, y), occ: 8 (over x, core).
Axes of the slice: x: 4, y: 4, z: 8, core: 2. Of those that a mesh axis runs over, the one named last changes fastest.
Arguments:
- ao_tiles: bfloat16 [5120, 8, 32, 128], P('task'), may hold values from -6 to 6
- mo_coeffs: bfloat16 [1536, 200], P(None, 'occ'), may hold values from -0.5 to 0.5
- mu_blocks: int32 [5120], P('task'), may hold values from 0 to 191
- nu_blocks: int32 [5120], P('task'), may hold values from 0 to 47
- tile_live: int32 [5120], P('task'), may hold values 0 or 1
- batch_target: int32 [640], P('task'), may hold values from 0 to 2
- batch_count: int32 [32], P('task'), may hold values from 1 to 20
Outputs:
- half_mo: float32 [200, 200, 4096], P('occ', None, 'task')
The draws below stay inside these ranges and needn't reach their ends.
Inputs may be any that keep to these rules, and one draw needn't show every extreme that they name: `batch_target`: the batch's kl block is the block owned by task index (own index + value) mod 32. `batch_count`: batches at or after this count in a list are not part of the work.
All inputs are finite; a program needn't handle non-finite values. No bound on the sum of `tile_live` on one device may be relied on, other than what follows from the above.
Results may differ from the reference program's by a relative error of at most 0.0029.
Values may be sent and summed in bfloat16 or wider, within the bound.
A program may use at most 128 MiB of HBM per device.

```python
import jax
import jax.numpy as jnp
from jax import lax

NBF = 1536
NOCC = 200
MUT = 8
NUT = 32
KLW = 128
BATCH = 8
NB = 20
SPREAD = 3
BLOCKS = 640
TILES = 5120
N_TASK = 32


def with_ends(result, rng, smallest, largest):
    index_at = [jax.random.randint(jax.random.fold_in(rng, axis), (), 0, length) for axis, length in enumerate(result.shape)]
    widest = result.shape.index(max(result.shape))
    neighbour = index_at[:widest] + [(index_at[widest] + 1) % result.shape[widest]] + index_at[widest + 1:]
    return result.at[tuple(index_at)].set(smallest).at[tuple(neighbour)].set(largest)


def steps_of(own_key, shape, cuts, least, high):
    gain, own = 1.0, jax.random.fold_in(own_key, 6)
    for dim, shards_of in cuts:
        heights = jnp.exp(jax.random.uniform(jax.random.fold_in(own, dim), (shards_of,), jnp.float32, least / len(cuts), high / len(cuts)))
        gain = gain * jnp.repeat(heights, shape[dim] // shards_of).reshape([-1 if axis == dim else 1 for axis in range(len(shape))])
    return gain


def scatter_about(own_key, dims, spread, reach, split=(), held_as=jnp.bfloat16):
    level = steps_of(own_key, dims, split, -0.22, 0.18) if split else 1.0
    array = jax.random.normal(own_key, dims, jnp.float32) * spread * level
    return jnp.minimum(jnp.maximum(array, -reach), reach).astype(held_as)


def setup_inputs(seed: int = 0) -> dict:
    key_list = jax.random.split(jax.random.key(seed), 8)
    return {
        "ao_tiles": scatter_about(key_list[0], (TILES, MUT, NUT, KLW), 1.0, 6.0, ((0, 32),)),
        "mo_coeffs": scatter_about(key_list[1], (NBF, NOCC), 128 ** -0.5, 0.5, ((1, 8),)),
        "mu_blocks": with_ends(jax.random.randint(key_list[2], (TILES,), 0, NBF // MUT), jax.random.fold_in(key_list[2], 1), 0, (NBF // MUT) - 1).astype(jnp.int32),
        "nu_blocks": with_ends(jax.random.randint(key_list[3], (TILES,), 0, NBF // NUT), jax.random.fold_in(key_list[3], 1), 0, (NBF // NUT) - 1).astype(jnp.int32),
        "tile_live": with_ends((jax.random.randint(key_list[4], (TILES,), 0, 4) < 3).astype(jnp.int32), jax.random.fold_in(key_list[4], 1), 0, 1),
        "batch_target": with_ends(jax.random.randint(key_list[5], (BLOCKS,), 0, SPREAD), jax.random.fold_in(key_list[5], 1), 0, SPREAD - 1).astype(jnp.int32),
        "batch_count": with_ends(jax.random.randint(key_list[6], (N_TASK,), 1, NB + 1), jax.random.fold_in(key_list[6], 1), 1, NB).astype(jnp.int32),
    }


def reference(ao_tiles, mo_coeffs, mu_blocks, nu_blocks, tile_live, batch_target, batch_count):
    coeff_full = mo_coeffs.astype(jnp.float32)
    tiles_all = ao_tiles.reshape(N_TASK, NB, BATCH, MUT, NUT, KLW)
    mu_all = mu_blocks.reshape(N_TASK, NB, BATCH)
    nu_all = nu_blocks.reshape(N_TASK, NB, BATCH)
    live_all = tile_live.reshape(N_TASK, NB, BATCH)
    target_all = batch_target.reshape(N_TASK, NB)
    mu_offsets = jnp.arange(MUT, dtype=jnp.int32)
    nu_offsets = jnp.arange(NUT, dtype=jnp.int32)
    spread_ids = jnp.arange(SPREAD, dtype=jnp.int32)

    def one_group(output, group_items):
        tiles_g, mu_g, nu_g, live_g, target_g, listed, group_index = group_items

        def one_batch(partials, batch_items):
            tile_block, mu_ids, nu_ids, live_ids, target, batch_index = batch_items
            coeff_mu = coeff_full[mu_ids[:, None] * MUT + mu_offsets[None, :]]
            quarter = jnp.einsum("bmi,bmnk->bink", coeff_mu, tile_block.astype(jnp.float32)).astype(jnp.bfloat16)
            kept_tiles = (live_ids * (batch_index < listed).astype(jnp.int32)).astype(jnp.float32)
            coeff_nu = coeff_full[nu_ids[:, None] * NUT + nu_offsets[None, :]] * kept_tiles[:, None, None]
            contribution = jnp.einsum("bnj,bink->ijk", coeff_nu, quarter.astype(jnp.float32))
            chosen = (spread_ids == target).astype(jnp.float32)
            return partials + chosen[:, None, None, None] * contribution[None], None

        initial = jnp.zeros((SPREAD, NOCC, NOCC, KLW), jnp.float32)
        partials = lax.scan(one_batch, initial, (tiles_g, mu_g, nu_g, live_g, target_g, jnp.arange(NB, dtype=jnp.int32)))[0]
        for spread_index in range(SPREAD):
            owner_index = (group_index + spread_index) % N_TASK
            column = (owner_index * KLW).astype(jnp.int32)
            earlier = lax.dynamic_slice_in_dim(output, column, KLW, 2)
            output = lax.dynamic_update_slice_in_dim(output, earlier + partials[spread_index], column, 2)
        return output, None

    output = jnp.zeros((NOCC, NOCC, N_TASK * KLW), jnp.float32)
    output = lax.scan(one_group, output, (tiles_all, mu_all, nu_all, live_all, target_all, batch_count, jnp.arange(N_TASK, dtype=jnp.int32)))[0]
    return output
```

```python
from functools import partial

import jax
import jax.numpy as jnp
from jax import lax
from jax.experimental import pallas as pl
from jax.experimental.pallas import tpu as pltpu
from jax.sharding import PartitionSpec as P

SPREAD = 3
MUT, NUT, KLW = 8, 32, 128
NB, BATCH = 20, 8
LANES = 256


def batch_kernel(
    targets, first, width,
    mu_ref, nu_ref, live_ref, target_ref, count_ref, tiles_hbm, spread_ref, coeff_ref,
    *rest,
):
    out_refs = rest[: len(targets)]
    order, tiles, rows_nu, quarter, total, sem = rest[len(targets):]
    n_occ = 200
    local_occ = 25
    listed = count_ref[0]
    found = jnp.int32(0)
    ends = []
    for s in targets:
        def scan(b, found):
            hit = jnp.logical_and(b < listed, target_ref[b] == s)

            @pl.when(hit)
            def _():
                order[found] = b

            return found + hit.astype(jnp.int32)

        found = lax.fori_loop(0, NB, scan, found)
        ends.append(found)
    last = found

    def fetch(position, slot):
        return pltpu.make_async_copy(
            tiles_hbm.at[pl.ds(order[position] * BATCH, BATCH)], tiles.at[slot], sem.at[slot]
        )

    @pl.when(last > 0)
    def _():
        fetch(0, 0).start()

    row = lax.broadcasted_iota(jnp.int32, (16, 128), 0)
    lane = lax.broadcasted_iota(jnp.int32, (16, 128), 1)
    diagonal = (lane % 16 == row).astype(jnp.float32).astype(jnp.bfloat16)

    def visit(position, carry):
        slot = position % 2
        fetch(position, slot).wait()

        @pl.when(position + 1 < last)
        def _():
            fetch(position + 1, 1 - slot).start()

        batch = order[position]
        for t in range(BATCH):
            g = batch * BATCH + t
            base = mu_ref[g] * local_occ + first
            left = jnp.concatenate(
                [
                    jnp.broadcast_to(spread_ref[pl.ds(base + i, 1), :], (16, 128)).astype(
                        jnp.bfloat16
                    )
                    * diagonal
                    for i in range(width)
                ],
                axis=0,
            )
            block = tiles[slot, t]
            right = jnp.concatenate(
                [block[:, 16 * q : 16 * q + 16].reshape(128, 128) for q in range(2)], axis=1
            )
            product = jnp.dot(left, right, preferred_element_type=jnp.float32)
            product = product.astype(jnp.bfloat16).reshape(width, 16, 256)
            for q in range(2):
                quarter[:, 32 * t + 16 * q : 32 * t + 16 * q + 16, :] = product[
                    :, :, 128 * q : 128 * q + 128
                ]
            nu_rows = coeff_ref[pl.ds(pl.multiple_of(nu_ref[g] * NUT, NUT), NUT), :]
            rows_nu[32 * t : 32 * t + 32, :] = nu_rows * live_ref[g].astype(
                jnp.float32
            ).astype(jnp.bfloat16)
        across = rows_nu[...].T[:n_occ]
        for i in range(0, width, 2):
            if i + 1 < width:
                right = jnp.concatenate([quarter[i], quarter[i + 1]], axis=1)
            else:
                right = quarter[i]
            product = jnp.dot(across, right, preferred_element_type=jnp.float32)
            total[i] += product[:, :128]
            if i + 1 < width:
                total[i + 1] += product[:, 128:]
        return carry

    start = jnp.int32(0)
    for s, end, out_ref in zip(targets, ends, out_refs):
        total[...] = jnp.zeros_like(total)
        lax.fori_loop(start, end, visit, 0)
        out_ref[...] = total[...].astype(out_ref.dtype)
        start = end


def batches(targets, first, width, dtype, scalars, tiles, spread, coeff):
    smem = pl.BlockSpec(memory_space=pltpu.SMEM)
    vmem = pl.BlockSpec(memory_space=pltpu.VMEM)
    shape = jax.ShapeDtypeStruct((width, 200, KLW), dtype)
    return pl.pallas_call(
        partial(batch_kernel, targets, first, width),
        out_shape=[shape] * len(targets),
        in_specs=[smem] * 5 + [pl.BlockSpec(memory_space=pl.ANY), vmem, vmem],
        out_specs=[vmem] * len(targets),
        scratch_shapes=[
            pltpu.SMEM((NB,), jnp.int32),
            pltpu.VMEM((2, BATCH, MUT, NUT, KLW), jnp.bfloat16),
            pltpu.VMEM((256, LANES), jnp.bfloat16),
            pltpu.VMEM((width, 256, KLW), jnp.bfloat16),
            pltpu.VMEM((width, 200, KLW), jnp.float32),
            pltpu.SemaphoreType.DMA((2,)),
        ],
        compiler_params=pltpu.CompilerParams(vmem_limit_bytes=40 << 20),
        cost_estimate=pl.CostEstimate(
            flops=len(targets) * width * 60_000_000, bytes_accessed=10_000_000, transcendentals=0
        ),
    )(*scalars, tiles, spread, coeff)


def hop(array, side, wrap_rows):
    route = []
    for t in range(32):
        z, y = divmod(t, 4)
        z = (z + (1 if y in wrap_rows else 0)) % 8
        route.append((t, z * 4 + (y + side) % 4))
    return lax.ppermute(array, "task", route)


CHUNKS = ((0, 5, True), (5, 10, False), (15, 10, False))


def local(ao_tiles, mo_coeffs, mu_blocks, nu_blocks, tile_live, batch_target, batch_count):
    coeff_all = lax.all_gather(mo_coeffs.T, "occ", axis=0, tiled=True).T
    coeff_all = jnp.pad(coeff_all, ((0, 0), (0, LANES - coeff_all.shape[1])))
    spread = jnp.broadcast_to(
        mo_coeffs.reshape(192, MUT, 25).transpose(0, 2, 1)[..., None].astype(jnp.float32), (192, 25, MUT, 16)
    ).reshape(192 * 25, 128)
    scalars = (mu_blocks, nu_blocks, tile_live, batch_target, batch_count)
    forward, backward = [], []
    for first, width, chained in CHUNKS:
        two, one = batches((2, 1), first, width, jnp.bfloat16, scalars, ao_tiles, spread, coeff_all)
        if chained:
            two = hop(two, 1, (3,))
            one = (one.astype(jnp.float32) + two.astype(jnp.float32)).astype(jnp.bfloat16)
        else:
            two = hop(hop(two, -1, ()), -1, (1, 2))
            backward.append(two)
        forward.append(hop(one, 1, (3,)))
    zero, = batches((0,), 0, 25, jnp.float32, scalars, ao_tiles, spread, coeff_all)
    pieces = []
    for index, (first, width, chained) in enumerate(CHUNKS):
        piece = zero[first : first + width] + forward[index].astype(jnp.float32)
        if not chained:
            piece = piece + backward.pop(0).astype(jnp.float32)
        pieces.append(piece)
    return jnp.concatenate(pieces, axis=0)


def solution(mesh):
    in_specs = (
        P("task", None, None, None),
        P(None, "occ"),
        P("task"),
        P("task"),
        P("task"),
        P("task"),
        P("task"),
    )
    out_specs = P("occ", None, "task")
    return jax.shard_map(local, mesh=mesh, in_specs=in_specs, out_specs=out_specs, check_vma=False)
```

```python
import jax
import jax.numpy as jnp
from jax import lax
from jax.experimental import pallas as pl
from jax.experimental.pallas import tpu as pltpu
from jax.sharding import PartitionSpec as P

MESH = pl.DeviceIdType.MESH
SPREAD, MUT, NUT, KLW = 3, 8, 32, 128
NB, BATCH = 20, 8
TILES = NB * BATCH
NOCC, LOCAL, BLOCKS_MU = 200, 25, 192
DEPTH = TILES * NUT
STEP = 16
PIECES = 5

VMEM_LIMIT = 60 << 20
WIDTH = 4
FULL = LOCAL // WIDTH
COUNT = FULL + 1
SPLIT = 128


def kernel(
    mu_ref, nu_ref, live_ref, target_ref, count_ref, own_ref, tiles_hbm, out_ref,
    tiles, spread, gathered, staged, turned, across, quarter, held, send_two, send_one, mid, from_one, from_two,
    load_sem, own_sem, gather_send, gather_recv, send_sem, recv_sem,
):
    task, occ = lax.axis_index("task"), lax.axis_index("occ")
    z, y = task // 4, task % 4
    up, down = (y + 1) % 4, (y + 3) % 4
    after = (task + 1) % 32
    before = (task + 31) % 32
    minus, minus_from = z * 4 + down, z * 4 + up
    jump = ((y + 1) // 2) % 2
    last_hop = ((z + jump) % 8) * 4 + down
    jumped = ((up + 1) // 2) % 2
    last_from = ((z + 8 - jumped) % 8) * 4 + up
    x, core = occ // 2, occ % 2
    partner = x * 2 + 1 - core

    per_piece = TILES // PIECES

    def load(piece):
        return pltpu.make_async_copy(
            tiles_hbm.at[pl.ds(piece * per_piece, per_piece)],
            tiles.at[pl.ds(piece * per_piece, per_piece)],
            load_sem.at[piece],
        )

    for piece in range(PIECES):
        load(piece).start()

    barrier = pltpu.get_barrier_semaphore()
    for other in (after, before, minus, minus_from, last_hop, last_from):
        pl.semaphore_signal(barrier, inc=1, device_id={"task": other}, device_id_type=MESH)
    for other in (partner, (x + 1) % 4 * 2 + core, (x + 2) % 4 * 2 + core, (x + 3) % 4 * 2 + core):
        pl.semaphore_signal(barrier, inc=1, device_id={"occ": other}, device_id_type=MESH)
    pl.semaphore_wait(barrier, 10)

    def give(source, slot, index, other):
        return pltpu.make_async_remote_copy(
            src_ref=source, dst_ref=gathered.at[core, slot],
            send_sem=gather_send.at[index], recv_sem=gather_recv.at[index],
            device_id={"occ": other}, device_id_type=MESH,
        )

    def direct(d):
        return give(own_ref, x, d, (x + d) % 4 * 2 + core)

    def across_chip(d):
        slot = (x + 4 - d) % 4
        return give(own_ref if d == 0 else gathered.at[core, slot], slot, 4 + d, partner)

    for d in (2, 1, 3):
        direct(d).start()
    across_chip(0).start()
    keep_own = pltpu.make_async_copy(own_ref, gathered.at[core, x], own_sem)
    keep_own.start()

    row = lax.broadcasted_iota(jnp.int32, (128, 128), 0)
    lane = lax.broadcasted_iota(jnp.int32, (128, 128), 1)
    spreader = jnp.concatenate(
        [
            jnp.where(row == lane // 16 + 8 * v, 1.0, 0.0).astype(jnp.bfloat16)
            for v in range(16)
        ],
        axis=1,
    )

    def spread_block(block, carry):
        part = own_ref[:, pl.ds(pl.multiple_of(block * 128, 128), 128)]
        wide = jnp.dot(part, spreader, preferred_element_type=jnp.float32)
        for v in range(16):
            spread[block * 16 + v, :LOCAL] = wide[:, 128 * v : 128 * v + 128]
        return carry

    lax.fori_loop(0, 12, spread_block, 0)

    row = lax.broadcasted_iota(jnp.int32, (16, 128), 0)
    lane = lax.broadcasted_iota(jnp.int32, (16, 128), 1)
    diagonal = jnp.where(lane % 16 == row, 1.0, 0.0).astype(jnp.bfloat16)

    def quarters(first, width, step):
        for u in range(STEP):
            g = step * STEP + u
            mu = mu_ref[g]
            left = jnp.concatenate(
                [
                    jnp.broadcast_to(spread[mu, pl.ds(first + i, 1), :], (16, 128)).astype(
                        jnp.bfloat16
                    )
                    * diagonal
                    for i in range(width)
                ],
                axis=0,
            )
            block = tiles[g]
            right = jnp.concatenate(
                [block[:, 16 * q : 16 * q + 16].reshape(128, 128) for q in range(2)], axis=1
            )
            product = jnp.dot(left, right, preferred_element_type=jnp.float32)
            product = product.astype(jnp.bfloat16).reshape(width, 16, 256)
            for q in range(2):
                quarter[:width, pl.ds(pl.multiple_of(g * 32 + 16 * q, 16), 16), :] = product[
                    :, :, 128 * q : 128 * q + 128
                ]

    def all_quarters(first, width):
        def inner(step, carry):
            quarters(first, width, step)
            return carry

        lax.fori_loop(0, TILES // STEP, inner, 0)

    for d in (1, 3, 2):
        direct(d).wait_recv()
        across_chip(d).start()
    for piece in range(PIECES):
        load(piece).wait()
    all_quarters(0, WIDTH)
    keep_own.wait()
    for d in range(4):
        across_chip(d).wait_recv()

    def turn(block, carry):
        where = pl.ds(pl.multiple_of(block * 128, 128), 128)
        for o in range(8):
            staged[25 * o : 25 * o + 25, :] = gathered[o % 2, o // 2, :, where].astype(jnp.float32)
        wide = staged[...]
        turned[0, block] = wide.astype(jnp.bfloat16)
        for r in range(1, 4):
            turned[r, block] = pltpu.roll(wide, 32 * r, 1).astype(jnp.bfloat16)
        return carry

    lax.fori_loop(0, 12, turn, 0)

    lanes = lax.broadcasted_iota(jnp.int32, (NOCC, 128), 1) // 32
    line = lax.broadcasted_iota(jnp.int32, (8, 128), 1) // 32
    listed = count_ref[0]

    def gather(group, carry):
        batch = group // 2
        merged = None
        kept = jnp.zeros((8, 128), jnp.int32)
        for u in range(4):
            g = group * 4 + u
            nu = nu_ref[g]
            part = turned[(u + 4 - nu % 4) % 4, nu // 4].astype(jnp.float32)
            merged = part if u == 0 else jnp.where(lanes == u, part, merged)
            kept = jnp.where(line == u, live_ref[g], kept)
        where = pl.ds(pl.multiple_of(group * 128, 128), 128)
        target = target_ref[batch]
        for s in range(SPREAD):
            chosen = jnp.where(target == s, jnp.where(batch < listed, 1, 0), 0)
            scale = (kept * chosen).astype(jnp.float32)[:1]
            across[s, :, where] = (merged * scale).astype(jnp.bfloat16)
        return carry

    lax.fori_loop(0, TILES // 4, gather, 0)

    def partial_sum(s, width):
        right = jnp.concatenate([quarter[i] for i in range(width)], axis=1)
        return jnp.dot(across[s], right, preferred_element_type=jnp.float32)

    def copy(source, target, kind, chunk, width, low, high, device):
        box = (pl.ds(chunk * WIDTH, width), pl.ds(low, high - low))
        return pltpu.make_async_remote_copy(
            src_ref=source.at[box], dst_ref=target.at[box],
            send_sem=send_sem.at[kind, chunk], recv_sem=recv_sem.at[kind, chunk],
            device_id={"task": device}, device_id_type=MESH,
        )

    def copy_one(chunk, width):
        return copy(send_one, from_one, 0, chunk, width, 0, SPLIT, after)

    def copy_two(chunk, width):
        return copy(send_two, mid, 1, chunk, width, 0, SPLIT, minus)

    def copy_on(chunk, width):
        return copy(mid, from_two, 2, chunk, width, 0, SPLIT, last_hop)

    def copy_through(chunk, width):
        return copy(send_two, mid, 3, chunk, width, SPLIT, NOCC, after)

    def copy_sum(chunk, width):
        return copy(send_one, from_one, 4, chunk, width, SPLIT, NOCC, after)

    def relay(chunk, width):
        copy_two(chunk, width).wait_recv()
        copy_on(chunk, width).start()
        copy_through(chunk, width).wait_recv()
        for i in range(width):
            at = chunk * WIDTH + i
            send_one[at, SPLIT:] = (held[at] + mid[at, SPLIT:].astype(jnp.float32)).astype(jnp.bfloat16)
        copy_sum(chunk, width).start()

    def finish(chunk, width):
        copy_one(chunk, width).wait_recv()
        copy_on(chunk, width).wait_recv()
        copy_sum(chunk, width).wait_recv()
        for i in range(width):
            at = chunk * WIDTH + i
            out_ref[at] = out_ref[at] + from_one[at].astype(jnp.float32)
            out_ref[at, :SPLIT] = out_ref[at, :SPLIT] + from_two[at, :SPLIT].astype(jnp.float32)

    def sums(chunk, width, between):
        total = partial_sum(2, width)
        for i in range(width):
            send_two[chunk * WIDTH + i] = total[:, 128 * i : 128 * i + 128].astype(jnp.bfloat16)
        copy_two(chunk, width).start()
        copy_through(chunk, width).start()
        between()
        total = partial_sum(1, width)
        for i in range(width):
            part = total[:, 128 * i : 128 * i + 128]
            send_one[chunk * WIDTH + i, :SPLIT] = part[:SPLIT].astype(jnp.bfloat16)
            held[chunk * WIDTH + i] = part[SPLIT:]
        copy_one(chunk, width).start()
        total = partial_sum(0, width)
        for i in range(width):
            out_ref[chunk * WIDTH + i] = total[:, 128 * i : 128 * i + 128]

    def body(chunk, carry):
        def between():
            @pl.when(chunk > 0)
            def _():
                relay(chunk - 1, WIDTH)

        sums(chunk, WIDTH, between)

        @pl.when(chunk < FULL - 1)
        def _():
            all_quarters(chunk * WIDTH + WIDTH, WIDTH)

        return carry

    lax.fori_loop(0, FULL, body, 0)
    all_quarters(FULL * WIDTH, 1)
    sums(FULL, 1, lambda: relay(FULL - 1, WIDTH))
    relay(FULL, 1)

    def ending(chunk, carry):
        finish(chunk, WIDTH)
        return carry

    lax.fori_loop(0, FULL, ending, 0)
    finish(FULL, 1)

    def sent(chunk, width):
        for copies in (copy_one, copy_two, copy_on, copy_through, copy_sum):
            copies(chunk, width).wait_send()

    def drain(chunk, carry):
        sent(chunk, WIDTH)
        return carry

    lax.fori_loop(0, FULL, drain, 0)
    sent(FULL, 1)
    for d in (1, 2, 3):
        direct(d).wait_send()
    for d in range(4):
        across_chip(d).wait_send()


def local(ao_tiles, mo_coeffs, mu_blocks, nu_blocks, tile_live, batch_target, batch_count):
    smem = pl.BlockSpec(memory_space=pltpu.SMEM)
    vmem = pl.BlockSpec(memory_space=pltpu.VMEM)
    lists = pltpu.VMEM((LOCAL, NOCC, KLW), jnp.bfloat16)
    return pl.pallas_call(
        kernel,
        out_shape=jax.ShapeDtypeStruct((LOCAL, NOCC, KLW), jnp.float32),
        in_specs=[smem] * 5 + [vmem, pl.BlockSpec(memory_space=pl.ANY)],
        out_specs=vmem,
        scratch_shapes=[
            pltpu.VMEM((TILES, MUT, NUT, KLW), jnp.bfloat16),
            pltpu.VMEM((BLOCKS_MU, 32, 128), jnp.float32),
            pltpu.VMEM((2, 4, LOCAL, BLOCKS_MU * MUT), jnp.bfloat16),
            pltpu.VMEM((NOCC, 128), jnp.float32),
            pltpu.VMEM((4, 12, NOCC, 128), jnp.bfloat16),
            pltpu.VMEM((SPREAD, NOCC, DEPTH), jnp.bfloat16),
            pltpu.VMEM((WIDTH, DEPTH, KLW), jnp.bfloat16),
            pltpu.VMEM((LOCAL, NOCC - SPLIT, KLW), jnp.float32),
            lists, lists, lists, lists, lists,
            pltpu.SemaphoreType.DMA((PIECES,)),
            pltpu.SemaphoreType.DMA,
            pltpu.SemaphoreType.DMA((8,)),
            pltpu.SemaphoreType.DMA((8,)),
            pltpu.SemaphoreType.DMA((5, COUNT)),
            pltpu.SemaphoreType.DMA((5, COUNT)),
        ],
        compiler_params=pltpu.CompilerParams(
            vmem_limit_bytes=VMEM_LIMIT, collective_id=0, has_side_effects=True
        ),
    )(mu_blocks, nu_blocks, tile_live, batch_target, batch_count, mo_coeffs.T, ao_tiles)


def solution(mesh):
    in_specs = (
        P("task", None, None, None),
        P(None, "occ"),
        P("task"),
        P("task"),
        P("task"),
        P("task"),
        P("task"),
    )
    out_specs = P("occ", None, "task")
    return jax.shard_map(local, mesh=mesh, in_specs=in_specs, out_specs=out_specs, check_vma=False)
```

```python
import jax
import jax.numpy as jnp
from jax import lax
from jax.experimental import pallas as pl
from jax.experimental.pallas import tpu as pltpu
from jax.sharding import PartitionSpec as P

MESH = pl.DeviceIdType.MESH
SPREAD, MUT, NUT, KLW = 3, 8, 32, 128
NB, BATCH = 20, 8
TILES = NB * BATCH
NOCC, LOCAL, BLOCKS_MU = 200, 25, 192
NBF = BLOCKS_MU * MUT
PADDED = 208
STEP = 32
PIECES = 5
VMEM_LIMIT = 49 << 20
WIDTH = 5
COUNT = LOCAL // WIDTH
PAIRS = NB // 2 + 1
FRONT = 128
REAR = NOCC - FRONT
HALF = NBF // 2


def kernel(
    mu_hbm, nu_hbm, live_hbm, target_hbm, count_ref, own_hbm, tiles_hbm, out_ref,
    mu_ref, nu_ref, live_ref, target_ref, spots, own_ref,
    tiles, spread, gathered, staged, turned, across, quarter, running,
    held_front, held_rear, x_out, x_in, y_out, y_in, a_out, a_in, m_out, m_in, f_in,
    place, order, keep, small_sem, load_sem, own_sem, gather_send, gather_recv, send_sem, recv_sem,
):
    task, occ = lax.axis_index("task"), lax.axis_index("occ")
    z, y = task // 4, task % 4
    after = (task + 1) % 32
    before = (task + 31) % 32
    minus = (z + (y // 2) * (1 - y % 2)) % 8 * 4 + (y + 3) % 4
    minus_from = (z + 8 - (1 - y // 2) * (y % 2)) % 8 * 4 + (y + 1) % 4
    x, core = occ // 2, occ % 2
    right, left, far = (x + 1) % 4, (x + 3) % 4, (x + 2) % 4
    partner = x * 2 + 1 - core

    small = [
        pltpu.make_async_copy(source, target, small_sem.at[n])
        for n, (source, target) in enumerate(
            (
                (own_hbm, own_ref),
                (mu_hbm, mu_ref),
                (nu_hbm, nu_ref),
                (live_hbm, live_ref),
                (target_hbm, target_ref),
            )
        )
    ]
    for one in small:
        one.start()
    barrier = pltpu.get_barrier_semaphore()
    for other in (after, before, minus, minus_from):
        pl.semaphore_signal(barrier, inc=1, device_id={"task": other}, device_id_type=MESH)
    for other in (partner, right * 2 + core, left * 2 + core, far * 2 + core):
        pl.semaphore_signal(barrier, inc=1, device_id={"occ": other}, device_id_type=MESH)

    per_piece = TILES // PIECES

    def load(piece):
        return pltpu.make_async_copy(
            tiles_hbm.at[pl.ds(piece * per_piece, per_piece)],
            tiles.at[pl.ds(piece * per_piece, per_piece)],
            load_sem.at[piece],
        )

    small[0].wait()
    pl.semaphore_wait(barrier, 8)

    def give(source, target, index, other):
        return pltpu.make_async_remote_copy(
            src_ref=source, dst_ref=target,
            send_sem=gather_send.at[index], recv_sem=gather_recv.at[index],
            device_id={"occ": other}, device_id_type=MESH,
        )

    direct = [
        give(own_ref, gathered.at[core, x], n, other * 2 + core)
        for n, other in enumerate((right, left, far))
    ]
    over = [
        give(own_ref if n == 3 else gathered.at[core, slot], gathered.at[core, slot], 3 + n, partner)
        for n, slot in enumerate((left, right, far, x))
    ]
    for one in (direct[2], direct[0], direct[1], over[3]):
        one.start()
    keep_own = pltpu.make_async_copy(own_ref, gathered.at[core, x], own_sem)
    keep_own.start()
    for piece in range(PIECES):
        load(piece).start()

    row = lax.broadcasted_iota(jnp.int32, (128, 128), 0)
    lane = lax.broadcasted_iota(jnp.int32, (128, 128), 1)
    spreader = jnp.concatenate(
        [
            jnp.where(row == lane // 16 + 8 * v, 1.0, 0.0).astype(jnp.bfloat16)
            for v in range(16)
        ],
        axis=1,
    )

    def spread_block(block, carry):
        part = own_ref[:, pl.ds(pl.multiple_of(block * 128, 128), 128)]
        wide = jnp.dot(part, spreader, preferred_element_type=jnp.float32)
        for v in range(16):
            spread[block * 16 + v, :LOCAL] = wide[:, 128 * v : 128 * v + 128]
        return carry

    lax.fori_loop(0, 12, spread_block, 0)
    for n in range(2):
        direct[n].wait_recv()
        over[n].start()
    for one in small[1:]:
        one.wait()

    def spot(group, carry):
        for u in range(4):
            nu = nu_ref[group * 4 + u]
            turns = lax.rem(u + 4 - lax.rem(nu, 4), 4)
            spots[group * 4 + u] = turns * 12 + lax.div(nu, 4)
        return carry

    lax.fori_loop(0, TILES // 4, spot, 0)

    listed = count_ref[0]

    def count(b, found):
        t = target_ref[b]
        inside = jnp.where(b < listed, 1, 0)
        return tuple(n + jnp.where(t == s, inside, 0) for s, n in enumerate(found))

    zero = jnp.int32(0)
    found = lax.fori_loop(0, NB, count, (zero, zero, zero))
    pairs = [lax.div(n + 1, 2) for n in found]
    first_one, first_zero = pairs[2], pairs[2] + pairs[1]
    bases = (2 * first_zero, 2 * first_one, zero)

    def rank(b, seen):
        t = target_ref[b]
        inside = jnp.where(b < listed, 1, 0)
        at = jnp.where(t == 2, seen[2], jnp.where(t == 1, seen[1], seen[0]))
        place[b] = jnp.where(b < listed, at, -1)
        return tuple(n + jnp.where(t == s, inside, 0) for s, n in enumerate(seen))

    lax.fori_loop(0, NB, rank, bases)

    def fill(p, carry):
        held_by = jnp.int32(NB)
        for b in range(NB):
            held_by = jnp.where(place[b] == p, b, held_by)
        order[p] = held_by
        return carry

    lax.fori_loop(0, 2 * PAIRS, fill, 0)

    def runs(q, carry):
        fresh = jnp.where(q == first_one, 1, jnp.where(q == first_zero, 1, 0))
        keep[q] = (1 - fresh).astype(jnp.float32)
        return carry

    lax.fori_loop(0, PAIRS, runs, 0)
    ends = (first_zero + pairs[0], first_zero, first_one)
    final = [jnp.maximum(end - 1, 0) for end in ends]
    some = [jnp.where(n > 0, 1, 0).astype(jnp.float32) for n in pairs]


    row = lax.broadcasted_iota(jnp.int32, (16, 128), 0)
    lane = lax.broadcasted_iota(jnp.int32, (16, 128), 1)
    diagonal = jnp.where(lane % 16 == row, 1.0, 0.0).astype(jnp.bfloat16)

    def all_quarters(chunk):
        first = chunk * WIDTH
        slot = chunk % 2

        def inner(step, carry):
            for u in range(STEP):
                g = step * STEP + u
                mu = mu_ref[g]
                wide = jnp.concatenate(
                    [
                        jnp.broadcast_to(spread[mu, pl.ds(first + i, 1), :], (16, 128)).astype(
                            jnp.bfloat16
                        )
                        * diagonal
                        for i in range(WIDTH)
                    ],
                    axis=0,
                )
                block = tiles[g]
                both = jnp.concatenate(
                    [block[:, 16 * q : 16 * q + 16].reshape(128, 128) for q in range(2)], axis=1
                )
                product = jnp.dot(wide, both, preferred_element_type=jnp.float32)
                product = product.astype(jnp.bfloat16).reshape(WIDTH, 16, 256)
                for q in range(2):
                    start = u % BATCH * NUT + 16 * q
                    quarter[slot, :, step * (STEP // BATCH) + u // BATCH, start : start + 16, :] = product[
                        :, :, 128 * q : 128 * q + 128
                    ]
            return carry

        lax.fori_loop(0, TILES // STEP, inner, 0)

    for piece in range(PIECES):
        load(piece).wait()
    all_quarters(0)
    direct[2].wait_recv()
    over[2].start()
    all_quarters(1)
    keep_own.wait()
    for one in over:
        one.wait_recv()

    staged[NOCC:, :] = jnp.zeros((PADDED - NOCC, 128), jnp.float32)

    def turn(block, carry):
        where = pl.ds(pl.multiple_of(block * 128, 128), 128)
        for o in range(8):
            staged[25 * o : 25 * o + 25, :] = gathered[o % 2, o // 2, :, where].astype(jnp.float32)
        wide = staged[...]
        turned[block] = wide.astype(jnp.bfloat16)
        for r in range(1, 4):
            turned[r * 12 + block] = pltpu.roll(wide, 32 * r, 1).astype(jnp.bfloat16)
        return carry

    lax.fori_loop(0, 12, turn, 0)

    line = lax.broadcasted_iota(jnp.int32, (16, 128), 1) // 32
    quarter_lanes = [jnp.where(line == u, 1.0, 0.0) for u in range(4)]

    def gather(group, carry):
        merged = None
        for u in range(4):
            g = group * 4 + u
            mask = (quarter_lanes[u] * live_ref[g].astype(jnp.float32)).astype(jnp.bfloat16)
            mask = jnp.concatenate([mask] * (PADDED // 16), axis=0)
            part = turned[spots[g]] * mask
            merged = part if u == 0 else merged + part
        across[group // 2, group % 2] = merged
        return carry

    lax.fori_loop(0, TILES // 4, gather, 0)
    across[NB] = jnp.zeros((2, PADDED, 128), jnp.bfloat16)

    def all_sums(chunk):
        slot = chunk % 2
        for q in range(PAIRS):
            two = [order[2 * q + h] for h in range(2)]
            wide = jnp.concatenate([across[b, h] for b in two for h in range(2)], axis=1)
            rows = [jnp.minimum(b, NB - 1) for b in two]
            both = jnp.concatenate(
                [
                    jnp.concatenate([quarter[slot, i, at] for at in rows], axis=0)
                    for i in range(WIDTH)
                ],
                axis=1,
            )
            product = jnp.dot(wide, both, preferred_element_type=jnp.float32)
            for i in range(WIDTH):
                part = product[:NOCC, 128 * i : 128 * i + 128]
                if q > 0:
                    part = running[q - 1, i] * keep[q] + part
                running[q, i] = part

    def copy(source, target, kind, chunk, device):
        box = pl.ds(chunk * WIDTH, WIDTH)
        return pltpu.make_async_remote_copy(
            src_ref=source.at[box], dst_ref=target.at[box],
            send_sem=send_sem.at[kind, chunk], recv_sem=recv_sem.at[kind, chunk],
            device_id={"task": device}, device_id_type=MESH,
        )

    def copies(chunk):
        return (
            copy(x_out, x_in, 0, chunk, after),
            copy(y_out, y_in, 1, chunk, after),
            copy(a_out, a_in, 2, chunk, before),
            copy(m_out, m_in, 3, chunk, minus),
            copy(m_in, f_in, 4, chunk, minus),
        )

    def relay(chunk):
        send_x, send_y, send_a, send_m, _ = copies(chunk)
        send_a.wait_recv()
        for i in range(WIDTH):
            at = chunk * WIDTH + i
            m_out[at] = (held_rear[at] + a_in[at].astype(jnp.float32)).astype(jnp.bfloat16)
        send_m.start()
        send_x.wait_recv()
        for i in range(WIDTH):
            at = chunk * WIDTH + i
            y_out[at] = (held_front[at] + x_in[at].astype(jnp.float32)).astype(jnp.bfloat16)
        send_y.start()

    def forward(chunk):
        _, _, _, send_m, send_f = copies(chunk)
        send_m.wait_recv()
        send_f.start()

    def finish(chunk):
        _, send_y, _, _, send_f = copies(chunk)
        send_y.wait_recv()
        for i in range(WIDTH):
            at = chunk * WIDTH + i
            out_ref[at, :FRONT] = out_ref[at, :FRONT] + y_in[at].astype(jnp.float32)
        send_f.wait_recv()
        for i in range(WIDTH):
            at = chunk * WIDTH + i
            out_ref[at, FRONT:] = out_ref[at, FRONT:] + f_in[at].astype(jnp.float32)

    def body(chunk, carry):
        first = chunk * WIDTH

        all_sums(chunk)
        for i in range(WIDTH):
            two = running[final[2], i] * some[2]
            x_out[first + i] = two[:FRONT].astype(jnp.bfloat16)
            held_rear[first + i] = two[FRONT:]
        send_x, _, send_a, _, _ = copies(chunk)
        send_x.start()
        for i in range(WIDTH):
            one = running[final[1], i] * some[1]
            a_out[first + i] = one[FRONT:].astype(jnp.bfloat16)
            held_front[first + i] = one[:FRONT]
        send_a.start()
        for i in range(WIDTH):
            out_ref[first + i] = running[final[0], i] * some[0]

        @pl.when(chunk > 0)
        def _():
            relay(chunk - 1)

        @pl.when(chunk > 1)
        def _():
            forward(chunk - 2)

        @pl.when(jnp.logical_and(chunk > 0, chunk < COUNT - 1))
        def _():
            all_quarters(chunk + 1)

        return carry

    lax.fori_loop(0, COUNT, body, 0)
    relay(COUNT - 1)
    forward(COUNT - 2)

    def ending(chunk, carry):
        finish(chunk)
        return carry

    lax.fori_loop(0, COUNT - 2, ending, 0)
    forward(COUNT - 1)
    lax.fori_loop(COUNT - 2, COUNT, ending, 0)

    def drain(chunk, carry):
        for one in copies(chunk):
            one.wait_send()
        return carry

    lax.fori_loop(0, COUNT, drain, 0)
    for one in direct + over:
        one.wait_send()


def keep_out(array):
    return pltpu.with_memory_space_constraint(array, pltpu.HBM)


def local(ao_tiles, mo_coeffs, mu_blocks, nu_blocks, tile_live, batch_target, batch_count):
    hbm = pl.BlockSpec(memory_space=pltpu.HBM)
    front = pltpu.VMEM((LOCAL, FRONT, KLW), jnp.bfloat16)
    rear = pltpu.VMEM((LOCAL, REAR, KLW), jnp.bfloat16)
    return pl.pallas_call(
        kernel,
        out_shape=jax.ShapeDtypeStruct((LOCAL, NOCC, KLW), jnp.float32),
        in_specs=[hbm] * 4 + [pl.BlockSpec(memory_space=pltpu.SMEM)] + [hbm] * 2,
        out_specs=pl.BlockSpec(memory_space=pltpu.VMEM),
        scratch_shapes=[
            pltpu.SMEM((TILES,), jnp.int32),
            pltpu.SMEM((TILES,), jnp.int32),
            pltpu.SMEM((TILES,), jnp.int32),
            pltpu.SMEM((NB,), jnp.int32),
            pltpu.SMEM((TILES,), jnp.int32),
            pltpu.VMEM((LOCAL, NBF), jnp.bfloat16),
            pltpu.VMEM((TILES, MUT, NUT, KLW), jnp.bfloat16),
            pltpu.VMEM((BLOCKS_MU, 32, 128), jnp.float32),
            pltpu.VMEM((2, 4, LOCAL, NBF), jnp.bfloat16),
            pltpu.VMEM((PADDED, 128), jnp.float32),
            pltpu.VMEM((48, PADDED, 128), jnp.bfloat16),
            pltpu.VMEM((NB + 1, 2, PADDED, 128), jnp.bfloat16),
            pltpu.VMEM((2, WIDTH, NB, BATCH * NUT, KLW), jnp.bfloat16),
            pltpu.VMEM((PAIRS, WIDTH, NOCC, KLW), jnp.float32),
            pltpu.VMEM((LOCAL, FRONT, KLW), jnp.float32),
            pltpu.VMEM((LOCAL, REAR, KLW), jnp.float32),
            front, front, front, front,
            rear, rear, rear, rear, rear,
            pltpu.SMEM((NB,), jnp.int32),
            pltpu.SMEM((2 * PAIRS,), jnp.int32),
            pltpu.SMEM((PAIRS,), jnp.float32),
            pltpu.SemaphoreType.DMA((5,)),
            pltpu.SemaphoreType.DMA((PIECES,)),
            pltpu.SemaphoreType.DMA,
            pltpu.SemaphoreType.DMA((7,)),
            pltpu.SemaphoreType.DMA((7,)),
            pltpu.SemaphoreType.DMA((5, COUNT)),
            pltpu.SemaphoreType.DMA((5, COUNT)),
        ],
        compiler_params=pltpu.CompilerParams(
            vmem_limit_bytes=VMEM_LIMIT, collective_id=0, has_side_effects=True
        ),
    )(keep_out(mu_blocks), keep_out(nu_blocks), keep_out(tile_live), keep_out(batch_target), batch_count, keep_out(mo_coeffs.T), ao_tiles)


def solution(mesh):
    in_specs = (
        P("task", None, None, None),
        P(None, "occ"),
        P("task"),
        P("task"),
        P("task"),
        P("task"),
        P("task"),
    )
    out_specs = P("occ", None, "task")
    return jax.shard_map(local, mesh=mesh, in_specs=in_specs, out_specs=out_specs, check_vma=False)
```

```python
import jax
import jax.numpy as jnp
from jax import lax
from jax.experimental import pallas as pl
from jax.experimental.pallas import tpu as pltpu
from jax.sharding import PartitionSpec as P

MESH = pl.DeviceIdType.MESH
SPREAD, MUT, NUT, KLW = 3, 8, 32, 128
NB, BATCH = 20, 8
TILES = NB * BATCH
NOCC, LOCAL, BLOCKS_MU = 200, 25, 192
NBF = BLOCKS_MU * MUT
PADDED = 208
STEP = 32
PIECES = 5
VMEM_LIMIT = 49 << 20
WIDTH = 5
COUNT = LOCAL // WIDTH
PAIRS = NB // 2 + 1
FRONT = 128
REAR = NOCC - FRONT
HALF = NBF // 2


def kernel(
    mu_hbm, nu_hbm, live_hbm, target_hbm, count_ref, own_hbm, tiles_hbm, out_ref,
    mu_ref, nu_ref, live_ref, target_ref, spots, own_ref,
    tiles, spread, gathered, staged, turned, across, quarter, running,
    held_front, held_rear, x_out, x_in, y_out, y_in, a_out, a_in, m_out, m_in, f_in,
    place, order, keep, small_sem, load_sem, own_sem, gather_send, gather_recv, send_sem, recv_sem,
):
    task, occ = lax.axis_index("task"), lax.axis_index("occ")
    z, y = task // 4, task % 4
    after = (task + 1) % 32
    before = (task + 31) % 32
    minus = (z + (y // 2) * (1 - y % 2)) % 8 * 4 + (y + 3) % 4
    minus_from = (z + 8 - (1 - y // 2) * (y % 2)) % 8 * 4 + (y + 1) % 4
    x, core = occ // 2, occ % 2
    right, left, far = (x + 1) % 4, (x + 3) % 4, (x + 2) % 4
    partner = x * 2 + 1 - core

    small = [
        pltpu.make_async_copy(source, target, small_sem.at[n])
        for n, (source, target) in enumerate(
            (
                (own_hbm, own_ref),
                (mu_hbm, mu_ref),
                (nu_hbm, nu_ref),
                (live_hbm, live_ref),
                (target_hbm, target_ref),
            )
        )
    ]
    for one in small:
        one.start()
    barrier = pltpu.get_barrier_semaphore()
    for other in (after, before, minus, minus_from):
        pl.semaphore_signal(barrier, inc=1, device_id={"task": other}, device_id_type=MESH)
    for other in (partner, right * 2 + core, left * 2 + core, far * 2 + core):
        pl.semaphore_signal(barrier, inc=1, device_id={"occ": other}, device_id_type=MESH)

    per_piece = TILES // PIECES

    def load(piece):
        return pltpu.make_async_copy(
            tiles_hbm.at[pl.ds(piece * per_piece, per_piece)],
            tiles.at[pl.ds(piece * per_piece, per_piece)],
            load_sem.at[piece],
        )

    small[0].wait()
    pl.semaphore_wait(barrier, 8)

    def give(source, target, index, other):
        return pltpu.make_async_remote_copy(
            src_ref=source, dst_ref=target,
            send_sem=gather_send.at[index], recv_sem=gather_recv.at[index],
            device_id={"occ": other}, device_id_type=MESH,
        )

    direct = [
        give(own_ref, gathered.at[core, x], n, other * 2 + core)
        for n, other in enumerate((right, left, far))
    ]
    over = [
        give(own_ref if n == 3 else gathered.at[core, slot], gathered.at[core, slot], 3 + n, partner)
        for n, slot in enumerate((left, right, far, x))
    ]
    for one in (direct[2], direct[0], direct[1], over[3]):
        one.start()
    keep_own = pltpu.make_async_copy(own_ref, gathered.at[core, x], own_sem)
    keep_own.start()
    for piece in range(PIECES):
        load(piece).start()

    row = lax.broadcasted_iota(jnp.int32, (128, 128), 0)
    lane = lax.broadcasted_iota(jnp.int32, (128, 128), 1)
    spreader = jnp.concatenate(
        [
            jnp.where(row == lane // 16 + 8 * v, 1.0, 0.0).astype(jnp.bfloat16)
            for v in range(16)
        ],
        axis=1,
    )

    def spread_block(block, carry):
        part = own_ref[:, pl.ds(pl.multiple_of(block * 128, 128), 128)]
        wide = jnp.dot(part, spreader, preferred_element_type=jnp.float32)
        for v in range(16):
            spread[block * 16 + v, :LOCAL] = wide[:, 128 * v : 128 * v + 128]
        return carry

    lax.fori_loop(0, 12, spread_block, 0)
    for n in range(2):
        direct[n].wait_recv()
        over[n].start()
    for one in small[1:]:
        one.wait()

    def spot(group, carry):
        for u in range(4):
            nu = nu_ref[group * 4 + u]
            turns = lax.rem(u + 4 - lax.rem(nu, 4), 4)
            spots[group * 4 + u] = turns * 12 + lax.div(nu, 4)
        return carry

    lax.fori_loop(0, TILES // 4, spot, 0)

    listed = count_ref[0]

    def count(b, found):
        t = target_ref[b]
        inside = jnp.where(b < listed, 1, 0)
        return tuple(n + jnp.where(t == s, inside, 0) for s, n in enumerate(found))

    zero = jnp.int32(0)
    found = lax.fori_loop(0, NB, count, (zero, zero, zero))
    pairs = [lax.div(n + 1, 2) for n in found]
    first_one, first_zero = pairs[2], pairs[2] + pairs[1]
    bases = (2 * first_zero, 2 * first_one, zero)

    def rank(b, seen):
        t = target_ref[b]
        inside = jnp.where(b < listed, 1, 0)
        at = jnp.where(t == 2, seen[2], jnp.where(t == 1, seen[1], seen[0]))
        place[b] = jnp.where(b < listed, at, -1)
        return tuple(n + jnp.where(t == s, inside, 0) for s, n in enumerate(seen))

    lax.fori_loop(0, NB, rank, bases)

    def fill(p, carry):
        held_by = jnp.int32(NB)
        for b in range(NB):
            held_by = jnp.where(place[b] == p, b, held_by)
        order[p] = held_by
        return carry

    lax.fori_loop(0, 2 * PAIRS, fill, 0)

    def runs(q, carry):
        fresh = jnp.where(q == first_one, 1, jnp.where(q == first_zero, 1, 0))
        keep[q] = (1 - fresh).astype(jnp.float32)
        return carry

    lax.fori_loop(0, PAIRS, runs, 0)
    ends = (first_zero + pairs[0], first_zero, first_one)
    final = [jnp.maximum(end - 1, 0) for end in ends]
    some = [jnp.where(n > 0, 1, 0).astype(jnp.float32) for n in pairs]


    row = lax.broadcasted_iota(jnp.int32, (16, 128), 0)
    lane = lax.broadcasted_iota(jnp.int32, (16, 128), 1)
    diagonal = jnp.where(lane % 16 == row, 1.0, 0.0).astype(jnp.bfloat16)

    def all_quarters(chunk):
        first = chunk * WIDTH
        slot = chunk % 2

        def inner(step, carry):
            for u in range(STEP):
                g = step * STEP + u
                mu = mu_ref[g]
                wide = jnp.concatenate(
                    [
                        jnp.broadcast_to(spread[mu, pl.ds(first + i, 1), :], (16, 128)).astype(
                            jnp.bfloat16
                        )
                        * diagonal
                        for i in range(WIDTH)
                    ],
                    axis=0,
                )
                block = tiles[g]
                both = jnp.concatenate(
                    [block[:, 16 * q : 16 * q + 16].reshape(128, 128) for q in range(2)], axis=1
                )
                product = jnp.dot(wide, both, preferred_element_type=jnp.float32)
                product = product.astype(jnp.bfloat16).reshape(WIDTH, 16, 256)
                for q in range(2):
                    start = u % BATCH * NUT + 16 * q
                    quarter[slot, :, step * (STEP // BATCH) + u // BATCH, start : start + 16, :] = product[
                        :, :, 128 * q : 128 * q + 128
                    ]
            return carry

        lax.fori_loop(0, TILES // STEP, inner, 0)

    for piece in range(PIECES):
        load(piece).wait()
    all_quarters(0)
    direct[2].wait_recv()
    over[2].start()
    all_quarters(1)
    keep_own.wait()
    for one in over:
        one.wait_recv()

    staged[NOCC:, :] = jnp.zeros((PADDED - NOCC, 128), jnp.float32)

    def turn(block, carry):
        where = pl.ds(pl.multiple_of(block * 128, 128), 128)
        for o in range(8):
            staged[25 * o : 25 * o + 25, :] = gathered[o % 2, o // 2, :, where].astype(jnp.float32)
        wide = staged[...]
        turned[block] = wide.astype(jnp.bfloat16).reshape(PADDED // 16, 16, 128)
        for r in range(1, 4):
            turned[r * 12 + block] = (
                pltpu.roll(wide, 32 * r, 1).astype(jnp.bfloat16).reshape(PADDED // 16, 16, 128)
            )
        return carry

    lax.fori_loop(0, 12, turn, 0)

    line = lax.broadcasted_iota(jnp.int32, (16, 128), 1) // 32
    quarter_lanes = [jnp.where(line == u, 1.0, 0.0) for u in range(4)]

    def gather(batch, carry):
        for half in range(2):
            merged = None
            for u in range(4):
                g = batch * BATCH + half * 4 + u
                mask = (quarter_lanes[u] * live_ref[g].astype(jnp.float32)).astype(jnp.bfloat16)
                mask = jnp.concatenate([mask[None]] * (PADDED // 16), axis=0)
                part = turned[spots[g]] * mask
                merged = part if u == 0 else merged + part
            across[batch, half] = merged
        return carry

    lax.fori_loop(0, NB, gather, 0)
    across[NB] = jnp.zeros((2, PADDED // 16, 16, 128), jnp.bfloat16)

    def all_sums(chunk):
        slot = chunk % 2
        for q in range(PAIRS):
            two = [order[2 * q + h] for h in range(2)]
            wide = jnp.concatenate([across[b, h].reshape(PADDED, 128) for b in two for h in range(2)], axis=1)
            rows = [jnp.minimum(b, NB - 1) for b in two]
            both = jnp.concatenate(
                [
                    jnp.concatenate([quarter[slot, i, at] for at in rows], axis=0)
                    for i in range(WIDTH)
                ],
                axis=1,
            )
            product = jnp.dot(wide, both, preferred_element_type=jnp.float32)
            for i in range(WIDTH):
                part = product[:NOCC, 128 * i : 128 * i + 128]
                if q > 0:
                    part = running[q - 1, i] * keep[q] + part
                running[q, i] = part

    def copy(source, target, kind, chunk, device):
        box = pl.ds(chunk * WIDTH, WIDTH)
        return pltpu.make_async_remote_copy(
            src_ref=source.at[box], dst_ref=target.at[box],
            send_sem=send_sem.at[kind, chunk], recv_sem=recv_sem.at[kind, chunk],
            device_id={"task": device}, device_id_type=MESH,
        )

    def copies(chunk):
        return (
            copy(x_out, x_in, 0, chunk, after),
            copy(y_out, y_in, 1, chunk, after),
            copy(a_out, a_in, 2, chunk, before),
            copy(m_out, m_in, 3, chunk, minus),
            copy(m_in, f_in, 4, chunk, minus),
        )

    def relay_rear(chunk):
        _, _, send_a, send_m, _ = copies(chunk)
        send_a.wait_recv()
        for i in range(WIDTH):
            at = chunk * WIDTH + i
            m_out[at] = (held_rear[at] + a_in[at].astype(jnp.float32)).astype(jnp.bfloat16)
        send_m.start()

    def relay_front(chunk):
        send_x, send_y, _, _, _ = copies(chunk)
        send_x.wait_recv()
        for i in range(WIDTH):
            at = chunk * WIDTH + i
            y_out[at] = (held_front[at] + x_in[at].astype(jnp.float32)).astype(jnp.bfloat16)
        send_y.start()

    def forward(chunk):
        _, _, _, send_m, send_f = copies(chunk)
        send_m.wait_recv()
        send_f.start()

    def finish(chunk):
        _, send_y, _, _, send_f = copies(chunk)
        send_y.wait_recv()
        for i in range(WIDTH):
            at = chunk * WIDTH + i
            out_ref[at, :FRONT] = out_ref[at, :FRONT] + y_in[at].astype(jnp.float32)
        send_f.wait_recv()
        for i in range(WIDTH):
            at = chunk * WIDTH + i
            out_ref[at, FRONT:] = out_ref[at, FRONT:] + f_in[at].astype(jnp.float32)

    def body(chunk, carry):
        first = chunk * WIDTH

        all_sums(chunk)
        for i in range(WIDTH):
            two = running[final[2], i] * some[2]
            x_out[first + i] = two[:FRONT].astype(jnp.bfloat16)
            held_rear[first + i] = two[FRONT:]
        send_x, _, send_a, _, _ = copies(chunk)
        send_x.start()
        for i in range(WIDTH):
            one = running[final[1], i] * some[1]
            a_out[first + i] = one[FRONT:].astype(jnp.bfloat16)
            held_front[first + i] = one[:FRONT]
        send_a.start()
        for i in range(WIDTH):
            out_ref[first + i] = running[final[0], i] * some[0]

        @pl.when(chunk > 0)
        def _():
            relay_front(chunk - 1)
            relay_rear(chunk - 1)

        @pl.when(jnp.logical_and(chunk > 0, chunk < COUNT - 1))
        def _():
            all_quarters(chunk + 1)

        @pl.when(chunk > 1)
        def _():
            forward(chunk - 2)

        return carry

    lax.fori_loop(0, COUNT, body, 0)
    relay_rear(COUNT - 1)
    relay_front(COUNT - 1)
    forward(COUNT - 2)

    def ending(chunk, carry):
        finish(chunk)
        return carry

    lax.fori_loop(0, COUNT - 2, ending, 0)
    forward(COUNT - 1)
    lax.fori_loop(COUNT - 2, COUNT, ending, 0)

    def drain(chunk, carry):
        for one in copies(chunk):
            one.wait_send()
        return carry

    lax.fori_loop(0, COUNT, drain, 0)
    for one in direct + over:
        one.wait_send()


def keep_out(array):
    return pltpu.with_memory_space_constraint(array, pltpu.HBM)


def local(ao_tiles, mo_coeffs, mu_blocks, nu_blocks, tile_live, batch_target, batch_count):
    hbm = pl.BlockSpec(memory_space=pltpu.HBM)
    front = pltpu.VMEM((LOCAL, FRONT, KLW), jnp.bfloat16)
    rear = pltpu.VMEM((LOCAL, REAR, KLW), jnp.bfloat16)
    return pl.pallas_call(
        kernel,
        out_shape=jax.ShapeDtypeStruct((LOCAL, NOCC, KLW), jnp.float32),
        in_specs=[hbm] * 4 + [pl.BlockSpec(memory_space=pltpu.SMEM)] + [hbm] * 2,
        out_specs=pl.BlockSpec(memory_space=pltpu.VMEM),
        scratch_shapes=[
            pltpu.SMEM((TILES,), jnp.int32),
            pltpu.SMEM((TILES,), jnp.int32),
            pltpu.SMEM((TILES,), jnp.int32),
            pltpu.SMEM((NB,), jnp.int32),
            pltpu.SMEM((TILES,), jnp.int32),
            pltpu.VMEM((LOCAL, NBF), jnp.bfloat16),
            pltpu.VMEM((TILES, MUT, NUT, KLW), jnp.bfloat16),
            pltpu.VMEM((BLOCKS_MU, 32, 128), jnp.float32),
            pltpu.VMEM((2, 4, LOCAL, NBF), jnp.bfloat16),
            pltpu.VMEM((PADDED, 128), jnp.float32),
            pltpu.VMEM((48, PADDED // 16, 16, 128), jnp.bfloat16),
            pltpu.VMEM((NB + 1, 2, PADDED // 16, 16, 128), jnp.bfloat16),
            pltpu.VMEM((2, WIDTH, NB, BATCH * NUT, KLW), jnp.bfloat16),
            pltpu.VMEM((PAIRS, WIDTH, NOCC, KLW), jnp.float32),
            pltpu.VMEM((LOCAL, FRONT, KLW), jnp.float32),
            pltpu.VMEM((LOCAL, REAR, KLW), jnp.float32),
            front, front, front, front,
            rear, rear, rear, rear, rear,
            pltpu.SMEM((NB,), jnp.int32),
            pltpu.SMEM((2 * PAIRS,), jnp.int32),
            pltpu.SMEM((PAIRS,), jnp.float32),
            pltpu.SemaphoreType.DMA((5,)),
            pltpu.SemaphoreType.DMA((PIECES,)),
            pltpu.SemaphoreType.DMA,
            pltpu.SemaphoreType.DMA((7,)),
            pltpu.SemaphoreType.DMA((7,)),
            pltpu.SemaphoreType.DMA((5, COUNT)),
            pltpu.SemaphoreType.DMA((5, COUNT)),
        ],
        compiler_params=pltpu.CompilerParams(
            vmem_limit_bytes=VMEM_LIMIT, collective_id=0, has_side_effects=True
        ),
    )(keep_out(mu_blocks), keep_out(nu_blocks), keep_out(tile_live), keep_out(batch_target), batch_count, keep_out(mo_coeffs.T), ao_tiles)


def solution(mesh):
    in_specs = (
        P("task", None, None, None),
        P(None, "occ"),
        P("task"),
        P("task"),
        P("task"),
        P("task"),
        P("task"),
    )
    out_specs = P("occ", None, "task")
    return jax.shard_map(local, mesh=mesh, in_specs=in_specs, out_specs=out_specs, check_vma=False)
```
